32 devices in a mesh: row: 4 (over y, x), col: 8 (over z, core).
Axes of the slice: x: 2, y: 2, z: 4, core: 2. Of those that a mesh axis runs over, the one named last changes fastest.
Arguments:
- pair_window: bfloat16 [8, 16, 32, 128], P('col', 'row'), may hold values from -6 to 6
- tri_cotangent: bfloat16 [8, 16, 128, 128], P(None, 'row', 'col'), may hold values from -0.75 to 0.75
- saved_left: bfloat16 [8, 16, 32, 128], P('col', 'row'), may hold values from -6 to 6
- saved_right: bfloat16 [8, 16, 32, 128], P('col', 'row'), may hold values from -6 to 6
- norm_gain: float32 [128], replicated, may hold values from 0.5 to 1.5
- norm_bias: float32 [128], replicated, may hold values from -3 to 3
- proj_weight: bfloat16 [4, 128, 128], replicated, may hold values from -0.5 to 0.5
Outputs:
- pair_grad: bfloat16 [8, 16, 32, 128], P('col', 'row')
- weight_grad: float32 [4, 128, 128], replicated
- norm_grad: float32 [2, 128], replicated
The draws below stay inside these ranges and needn't reach their ends.
All inputs are finite; a program needn't handle non-finite values.
Results may differ from the reference program's by a relative error of at most 0.0085.
Values may be sent and summed in bfloat16 or wider, within the bound.
A program may use at most 64 MiB of HBM per device.

```python
import jax
import jax.numpy as jnp
from jax import lax

C = 128
H = 128
K = 32
N_TOK = 128
BLOCKS = 8
TOK_BLOCK = 16


def raised(result, own_key, source, target, shards_of, factor):
    def block_of(position):
        return (jnp.arange(result.shape[position]) // (result.shape[position] // shards_of)).reshape((-1,) + (1,) * (result.ndim - 1 - position))

    near = jax.random.permutation(own_key, shards_of)[block_of(target)]
    far = (block_of(target) + shards_of // 2) % shards_of
    return jnp.where((block_of(source) == near) | (block_of(source) == far), factor * result, result)


def level_of(rng, extent, pieces, least, high):
    factor_of, own = 1.0, jax.random.fold_in(rng, 6)
    for dim, shards_of in pieces:
        draws = jnp.exp(jax.random.uniform(jax.random.fold_in(own, dim), (shards_of,), jnp.float32, least / len(pieces), high / len(pieces)))
        factor_of = factor_of * jnp.repeat(draws, extent[dim] // shards_of).reshape([-1 if axis == dim else 1 for axis in range(len(extent))])
    return factor_of


def normal_values(rng, extent, spread, limit, split=(), dtype=jnp.bfloat16):
    loudness = level_of(rng, extent, split, -0.22, 0.18) if split else 1.0
    values = jax.random.normal(rng, extent, jnp.float32) * spread * loudness
    return jnp.minimum(jnp.maximum(values, -limit), limit).astype(dtype)


def gaussian_with(key, extent, width, most, split, heavy, held_as=jnp.bfloat16):
    drawn = width * jax.random.normal(key, extent, jnp.float32)
    if split:
        drawn = drawn * level_of(key, extent, split, -0.22, 0.18)
    return jnp.clip(raised(drawn, jax.random.fold_in(key, 3), *heavy), -most, most).astype(held_as)


def setup_inputs(seed: int = 0) -> dict:
    arg_keys = jax.random.split(jax.random.key(seed), 8)
    pair_window = normal_values(arg_keys[0], (BLOCKS, TOK_BLOCK, K, C), 1.0, 6.0, ((0, 8), (1, 4)))
    tri_cotangent = gaussian_with(arg_keys[1], (BLOCKS, TOK_BLOCK, N_TOK, H), N_TOK ** -0.5, 0.75, ((1, 4), (2, 8)), (2, 0, 8, 2.0))
    saved_left = normal_values(arg_keys[2], (BLOCKS, TOK_BLOCK, K, H), 1.0, 6.0, ((0, 8), (1, 4)))
    saved_right = normal_values(arg_keys[3], (BLOCKS, TOK_BLOCK, K, H), 1.0, 6.0, ((0, 8), (1, 4)))
    norm_gain = jnp.clip(1.0 + 0.1 * jax.random.normal(arg_keys[4], (C,), jnp.float32), 0.5, 1.5)
    norm_bias = normal_values(arg_keys[5], (C,), 0.5, 3.0, (), jnp.float32)
    proj_weight = normal_values(arg_keys[6], (4, C, H), C ** -0.5, 0.5)
    return {"pair_window": pair_window, "tri_cotangent": tri_cotangent, "saved_left": saved_left, "saved_right": saved_right, "norm_gain": norm_gain, "norm_bias": norm_bias, "proj_weight": proj_weight}


def gated_norm_back(pair_rows, left_grad, right_grad, norm_gain, norm_bias, proj_weight):
    pair = pair_rows.astype(jnp.float32)
    average = lax.optimization_barrier(jnp.mean(pair, axis=-1, keepdims=True))
    centred = pair - average
    variance = lax.optimization_barrier(jnp.mean(centred * centred, axis=-1, keepdims=True))
    inv_std = lax.rsqrt(variance + 1e-05)
    unit_pair = centred * inv_std
    normed = (unit_pair * norm_gain + norm_bias).astype(jnp.bfloat16)
    chans = proj_weight.shape[2]
    stacked = jnp.transpose(proj_weight, (1, 0, 2)).reshape(proj_weight.shape[1], 4 * chans)
    preact = jnp.dot(normed, stacked, preferred_element_type=jnp.float32)
    gate_left = jax.nn.sigmoid(preact[:, :chans])
    value_left = preact[:, chans:2 * chans]
    gate_right = jax.nn.sigmoid(preact[:, 2 * chans:3 * chans])
    value_right = preact[:, 3 * chans:]
    pre_grads = jnp.concatenate([left_grad * value_left * gate_left * (1.0 - gate_left), left_grad * gate_left, right_grad * value_right * gate_right * (1.0 - gate_right), right_grad * gate_right], axis=1).astype(jnp.bfloat16)
    weight_part = lax.dot_general(normed, pre_grads, (((0,), (0,)), ((), ())), preferred_element_type=jnp.float32)
    weight_part = jnp.transpose(weight_part.reshape(proj_weight.shape[1], 4, chans), (1, 0, 2))
    normed_grad = jnp.dot(pre_grads, stacked.T, preferred_element_type=jnp.float32)
    norm_part = jnp.stack([lax.optimization_barrier(jnp.sum(normed_grad * unit_pair, axis=0)), lax.optimization_barrier(jnp.sum(normed_grad, axis=0))])
    scaled_grad = normed_grad * norm_gain
    pair_grad = inv_std * (scaled_grad - lax.optimization_barrier(jnp.mean(scaled_grad, axis=-1, keepdims=True)) - unit_pair * lax.optimization_barrier(jnp.mean(scaled_grad * unit_pair, axis=-1, keepdims=True)))
    return (pair_grad.astype(jnp.bfloat16), weight_part, norm_part)

def reference(pair_window, tri_cotangent, saved_left, saved_right, norm_gain, norm_bias, proj_weight):
    cotangent = tri_cotangent.reshape(N_TOK, N_TOK, H).astype(jnp.float32)
    left = saved_left.reshape(N_TOK, K, H).astype(jnp.float32)
    right = saved_right.reshape(N_TOK, K, H).astype(jnp.float32)
    left_grad = jnp.einsum('ijh,jkh->ikh', cotangent, right)
    right_grad = jnp.einsum('ijh,ikh->jkh', cotangent, left)
    pair_grad, weight_grad, norm_grad = gated_norm_back(pair_window.reshape(N_TOK * K, C), left_grad.reshape(N_TOK * K, H), right_grad.reshape(N_TOK * K, H), norm_gain, norm_bias, proj_weight)
    return (pair_grad.reshape(BLOCKS, TOK_BLOCK, K, C), weight_grad, norm_grad)
```

```python
import functools

import jax
import jax.numpy as jnp
from jax import lax
from jax.experimental import pallas as pl
from jax.experimental.pallas import tpu as pltpu
from jax.sharding import PartitionSpec as P

MESH = pl.DeviceIdType.MESH
F32 = jnp.float32
BF16 = jnp.bfloat16


def kernel(
    R,
    C,
    fused,
    z_hbm,
    dt_hbm,
    a_hbm,
    b_hbm,
    gain_hbm,
    bias_hbm,
    w_hbm,
    pair_ref,
    wgrad_ref,
    norm_ref,
    z_ref,
    dt_ref,
    a_ref,
    b_ref,
    gain_ref,
    bias_ref,
    w_ref,
    dt_other,
    dtf,
    a_all,
    b_all,
    ga_send,
    gb_send,
    ga_all,
    gb_all,
    coef,
    xhat_ref,
    normt_ref,
    inv_ref,
    wsend,
    wrecv,
    wback,
    nrecv,
    in_sem,
    dt_sem,
    a_ssem,
    a_rsem,
    b_ssem,
    b_rsem,
    ga_ssem,
    ga_rsem,
    gb_ssem,
    gb_rsem,
    ws_ssem,
    ws_rsem,
    wb_ssem,
    wb_rsem,
    n_ssem,
    n_rsem,
):
    r, c = lax.axis_index("row"), lax.axis_index("col")
    Z, N = C // 2, R * C
    z, q = c // 2, c % 2
    me = r * C + c
    T = a_ref.shape[1]
    K, H = a_ref.shape[2], a_ref.shape[3]
    KH = K // 2
    J = R * T

    def where(d):
        return (d // C, d % C)

    col_peers = [(s, lax.rem(c + s, C)) for s in range(1, C)]
    row_peers = [lax.rem(r + s, R) for s in range(1, R)]

    barrier = pltpu.get_barrier_semaphore()
    if fused:
        for s in range(1, N):
            pl.semaphore_signal(barrier, 1, device_id=where(lax.rem(me + s, N)), device_id_type=MESH)
        expected = N - 1
    else:
        for _, cc in col_peers:
            pl.semaphore_signal(barrier, 1, device_id=(r, cc), device_id_type=MESH)
        for rr in row_peers:
            for p in range(2):
                pl.semaphore_signal(barrier, 1, device_id=(rr, z * 2 + p), device_id_type=MESH)
        expected = C - 1 + 2 * (R - 1)

    loads = []
    for n, (src, dst) in enumerate(
        (
            (a_hbm, a_ref),
            (b_hbm, b_ref),
            (dt_hbm, dt_ref),
            (z_hbm, z_ref),
            (gain_hbm, gain_ref),
            (bias_hbm, bias_ref),
            (w_hbm, w_ref),
        )
    ):
        load = pltpu.make_async_copy(src, dst, in_sem.at[n])
        load.start()
        loads.append(load)
    for load in loads[:3]:
        load.wait()
    pl.semaphore_wait(barrier, expected)

    def remote(src, dst, ssem, rsem, dev):
        return pltpu.make_async_remote_copy(
            src_ref=src, dst_ref=dst, send_sem=ssem, recv_sem=rsem, device_id=dev, device_id_type=MESH
        )

    other = z * 2 + (1 - q)

    def half(p):
        return pl.ds(p * KH if isinstance(p, int) else pl.multiple_of(p * KH, KH), KH)

    sends = []

    def push(copy):
        copy.start()
        sends.append(copy)

    push(remote(dt_ref, dt_other, dt_sem.at[0], dt_sem.at[1], (r, other)))
    push(remote(b_ref.at[0, :, half(1 - q), :], b_all.at[q, pl.ds(r * T, T)], b_ssem.at[r, 1 - q], b_rsem.at[r, q], (r, other)))
    for rr in row_peers:
        for p in range(2):
            push(remote(b_ref.at[0, :, half(p), :], b_all.at[q, pl.ds(r * T, T)], b_ssem.at[rr, p], b_rsem.at[r, q], (rr, z * 2 + p)))
    for s in range(1, Z):
        zz = lax.rem(z + s, Z)
        for p in range(2):
            push(remote(a_ref.at[0, :, half(p), :], a_all.at[pl.ds(c * T, T)], a_ssem.at[zz * 2 + p], a_rsem.at[c], (r, zz * 2 + p)))
    push(remote(a_ref.at[0, :, half(1 - q), :], a_all.at[pl.ds(c * T, T)], a_ssem.at[other], a_rsem.at[c], (r, other)))

    for t in range(T):
        a_all[c * T + t] = a_ref[0, t, half(q), :]
        b_all[q, r * T + t] = b_ref[0, t, half(q), :]
    dtf[q] = dt_ref[...].reshape(C * T, J, H).astype(F32)

    for load in loads[3:]:
        load.wait()
    pair = z_ref[...].reshape(T * K, H).astype(F32)
    average = jnp.mean(pair, axis=-1, keepdims=True)
    centred = pair - average
    variance = jnp.mean(centred * centred, axis=-1, keepdims=True)
    inv_std = lax.rsqrt(variance + 1e-05)
    xhat = centred * inv_std
    normed32 = xhat * gain_ref[...] + bias_ref[...]
    normed = normed32.astype(BF16)
    normt_ref[...] = jnp.transpose(normed32).astype(BF16)
    xhat_ref[...] = xhat
    inv_ref[...] = jnp.broadcast_to(inv_std, inv_ref.shape)
    for m in range(2):
        gate = jax.nn.sigmoid(jnp.dot(normed, w_ref[2 * m], preferred_element_type=F32))
        value = jnp.dot(normed, w_ref[2 * m + 1], preferred_element_type=F32)
        coef[2 * m] = value * gate * (1.0 - gate)
        coef[2 * m + 1] = gate

    remote(dt_ref, dt_other, dt_sem.at[0], dt_sem.at[1], (r, other)).wait_recv()
    dtf[1 - q] = dt_other[...].reshape(C * T, J, H).astype(F32)

    def b_wait(rr, p):
        remote(b_all.at[p, pl.ds(rr * T, T)], b_all.at[p, pl.ds(rr * T, T)], b_ssem.at[rr, p], b_rsem.at[rr, p], (r, other)).wait_recv()

    b_wait(r, 1 - q)
    for rr in row_peers:
        for p in range(2):
            b_wait(rr, p)

    zero = jnp.zeros((KH, H), F32)
    for s in list(range(1, Z)) + [0]:
        zz = lax.rem(z + s, Z)
        acc = (zero,) * (2 * T)
        for core in range(2):

            def step(j, acc, core=core, zz=zz):
                right = b_all[core, j].astype(F32)
                return tuple(
                    acc[n] + dtf[core, zz * 2 * T + n, pl.ds(j, 1), :] * right for n in range(2 * T)
                )

            acc = lax.fori_loop(0, J, step, acc, unroll=4)
        if s:
            for p in range(2):
                for t in range(T):
                    ga_send[s, p, t] = acc[p * T + t].astype(BF16)
                push(remote(ga_send.at[s, p], ga_all.at[z, q], ga_ssem.at[s, p], ga_rsem.at[z, q], (r, zz * 2 + p)))
        else:
            for t in range(T):
                keep = jnp.where(q == 0, acc[t], acc[T + t])
                give = jnp.where(q == 0, acc[T + t], acc[t])
                ga_send[0, 0, t] = give.astype(BF16)
                ga_all[z, q, t] = keep.astype(BF16)
            push(remote(ga_send.at[0, 0], ga_all.at[z, q], ga_ssem.at[0, 0], ga_rsem.at[z, q], (r, other)))

    def a_wait(cc):
        remote(a_all.at[pl.ds(cc * T, T)], a_all.at[pl.ds(cc * T, T)], a_ssem.at[cc], a_rsem.at[cc], (r, other)).wait_recv()

    for _, cc in col_peers:
        a_wait(cc)
    for s in list(range(1, R)) + [0]:
        rr = lax.rem(r + s, R)

        def step(i, acc, rr=rr):
            left = a_all[i].astype(F32)
            return tuple(
                acc[n] + dtf[n // T, i, pl.ds(rr * T + n % T, 1), :] * left for n in range(2 * T)
            )

        acc = lax.fori_loop(0, C * T, step, (zero,) * (2 * T), unroll=4)
        if s:
            for p in range(2):
                for t in range(T):
                    gb_send[s, p, t] = acc[p * T + t].astype(BF16)
                push(remote(gb_send.at[s, p], gb_all.at[r, q], gb_ssem.at[s, p], gb_rsem.at[r, q], (rr, z * 2 + p)))
        else:
            for t in range(T):
                keep = jnp.where(q == 0, acc[t], acc[T + t])
                give = jnp.where(q == 0, acc[T + t], acc[t])
                gb_send[0, 0, t] = give.astype(BF16)
                gb_all[r, q, t] = keep.astype(BF16)
            push(remote(gb_send.at[0, 0], gb_all.at[r, q], gb_ssem.at[0, 0], gb_rsem.at[r, q], (r, other)))

    def total(buf, count):
        rows = []
        for t in range(T):
            for p in range(2):
                acc = buf[0, p, t].astype(F32)
                for n in range(1, count):
                    acc = acc + buf[n, p, t].astype(F32)
                rows.append(acc)
        return jnp.concatenate(rows, axis=0)

    def slot_wait(buf, sem, n, p):
        remote(buf.at[n, p], buf.at[n, p], dt_sem.at[0], sem.at[n, p], (r, other)).wait_recv()

    chunk = 4 * H // N if fused else 0
    normt = normt_ref[...]

    def weight_part(m, g):
        part = jnp.dot(normt, g, preferred_element_type=F32)
        if fused:
            per = part.shape[0] // chunk
            wsend[m * per : (m + 1) * per] = part.astype(BF16).reshape(per, chunk, H)
        else:
            wgrad_ref[m] = part

    def dn_part(m, g):
        return lax.dot_general(g, w_ref[m], (((1,), (1,)), ((), ())), preferred_element_type=F32)

    for s in list(range(1, Z)):
        zz = lax.rem(z + s, Z)
        for p in range(2):
            slot_wait(ga_all, ga_rsem, zz, p)
    slot_wait(ga_all, ga_rsem, z, 1 - q)
    left_grad = total(ga_all, Z)
    g = [(left_grad * coef[m]).astype(BF16) for m in range(2)]
    weight_part(0, g[0])
    weight_part(1, g[1])
    dn = dn_part(0, g[0]) + dn_part(1, g[1])

    for s in list(range(1, R)):
        rr = lax.rem(r + s, R)
        for p in range(2):
            slot_wait(gb_all, gb_rsem, rr, p)
    slot_wait(gb_all, gb_rsem, r, 1 - q)
    right_grad = total(gb_all, R)
    g = [(right_grad * coef[m]).astype(BF16) for m in range(2, 4)]
    weight_part(2, g[0])
    weight_part(3, g[1])
    if fused:
        for s in range(1, N):
            d = lax.rem(me + s, N)
            push(remote(wsend.at[d], wrecv.at[me], ws_ssem.at[s], ws_rsem.at[me], where(d)))
        wrecv[me] = wsend[me]
    dn = dn + dn_part(2, g[0]) + dn_part(3, g[1])

    xhat = xhat_ref[...]
    norm_part = jnp.concatenate(
        [jnp.sum(dn * xhat, axis=0, keepdims=True), jnp.sum(dn, axis=0, keepdims=True)], axis=0
    )
    if fused:
        nrecv[me] = norm_part
        for s in range(1, N):
            d = lax.rem(me + s, N)
            push(remote(nrecv.at[me], nrecv.at[me], n_ssem.at[s], n_rsem.at[me], where(d)))
    else:
        norm_ref[...] = norm_part
    dh = dn * gain_ref[...]
    grad = inv_ref[...] * (
        dh
        - jnp.mean(dh, axis=-1, keepdims=True)
        - xhat * jnp.mean(dh * xhat, axis=-1, keepdims=True)
    )
    pair_ref[...] = grad.astype(BF16).reshape(pair_ref.shape)

    if fused:
        for s in range(1, N):
            d = lax.rem(me + s, N)
            remote(wrecv.at[d], wrecv.at[d], ws_ssem.at[s], ws_rsem.at[d], where(d)).wait_recv()
        acc = wrecv[0].astype(F32)
        for n in range(1, N):
            acc = acc + wrecv[n].astype(F32)
        wback[me] = acc.astype(BF16)
        for s in range(1, N):
            d = lax.rem(me + s, N)
            push(remote(wback.at[me], wback.at[me], wb_ssem.at[s], wb_rsem.at[me], where(d)))
        for s in range(1, N):
            d = lax.rem(me + s, N)
            remote(nrecv.at[d], nrecv.at[d], n_ssem.at[s], n_rsem.at[d], where(d)).wait_recv()
        acc = nrecv[0]
        for n in range(1, N):
            acc = acc + nrecv[n]
        norm_ref[...] = acc
        for s in range(1, N):
            d = lax.rem(me + s, N)
            remote(wback.at[d], wback.at[d], wb_ssem.at[s], wb_rsem.at[d], where(d)).wait_recv()
        wgrad_ref[...] = wback[...].astype(F32).reshape(wgrad_ref.shape)
    for copy in sends:
        copy.wait_send()


def on_device(R, C, z, dt, a, b, gain, bias, w):
    _, T, K, H = a.shape
    J = dt.shape[2]
    KH, Z, N = K // 2, C // 2, R * C
    fused = (4 * H) % (16 * N) == 0
    M = N if fused else 1
    chunk = 4 * H // N if fused else 16
    V = pltpu.VMEM
    D = pltpu.SemaphoreType.DMA
    anyspace = pl.BlockSpec(memory_space=pl.ANY)
    vspace = pl.BlockSpec(memory_space=pltpu.VMEM)
    pair, wgrad, norm = pl.pallas_call(
        functools.partial(kernel, R, C, fused),
        out_shape=(
            jax.ShapeDtypeStruct(z.shape, BF16),
            jax.ShapeDtypeStruct(w.shape, F32),
            jax.ShapeDtypeStruct((2, z.shape[3]), F32),
        ),
        in_specs=[anyspace] * 7,
        out_specs=(vspace,) * 3,
        scratch_shapes=[
            V(z.shape, BF16),
            V(dt.shape, BF16),
            V(a.shape, BF16),
            V(b.shape, BF16),
            V((1, H), F32),
            V((1, H), F32),
            V(w.shape, BF16),
            V(dt.shape, BF16),
            V((2, C * T, J, H), F32),
            V((C * T, KH, H), BF16),
            V((2, J, KH, H), BF16),
            V((Z, 2, T, KH, H), BF16),
            V((R, 2, T, KH, H), BF16),
            V((Z, 2, T, KH, H), BF16),
            V((R, 2, T, KH, H), BF16),
            V((4, T * K, H), F32),
            V((T * K, H), F32),
            V((H, T * K), BF16),
            V((T * K, H), F32),
            V((M, chunk, H), BF16),
            V((M, chunk, H), BF16),
            V((M, chunk, H), BF16),
            V((M, 2, H), F32),
            D((7,)),
            D((2,)),
            D((C,)),
            D((C,)),
            D((R, 2)),
            D((R, 2)),
            D((Z, 2)),
            D((Z, 2)),
            D((R, 2)),
            D((R, 2)),
            D((M,)),
            D((M,)),
            D((M,)),
            D((M,)),
            D((M,)),
            D((M,)),
        ],
        compiler_params=pltpu.CompilerParams(
            collective_id=0, has_side_effects=True, vmem_limit_bytes=56 * 1024 * 1024
        ),
    )(z, dt, a, b, gain.reshape(1, -1), bias.reshape(1, -1), w)
    if not fused:
        wgrad, norm = lax.psum((wgrad, norm), ("row", "col"))
    return pair, wgrad, norm


def solution(mesh):
    R, C = mesh.shape["row"], mesh.shape["col"]
    return jax.shard_map(
        functools.partial(on_device, R, C),
        mesh=mesh,
        in_specs=(
            P("col", "row", None, None),
            P(None, "row", "col", None),
            P("col", "row", None, None),
            P("col", "row", None, None),
            P(),
            P(),
            P(),
        ),
        out_specs=(P("col", "row", None, None), P(), P()),
        check_vma=False,
    )
```

```python
import functools

import jax
import jax.numpy as jnp
from jax import lax
from jax.experimental import pallas as pl
from jax.experimental.pallas import tpu as pltpu
from jax.sharding import PartitionSpec as P

MESH = pl.DeviceIdType.MESH
F32 = jnp.float32
BF16 = jnp.bfloat16


def kernel(
    R,
    C,
    fused,
    z_hbm,
    dt_hbm,
    a_hbm,
    b_hbm,
    gain_hbm,
    bias_hbm,
    w_hbm,
    pair_ref,
    wgrad_ref,
    norm_ref,
    z_ref,
    dt_ref,
    a_ref,
    b_ref,
    gain_ref,
    bias_ref,
    w_ref,
    dt_other,
    dtf,
    a_all,
    b_all,
    ga_send,
    gb_send,
    ga_all,
    gb_all,
    coef,
    xhat_ref,
    normt_ref,
    inv_ref,
    wsend,
    wrecv,
    wback,
    nrecv,
    in_sem,
    dt_sem,
    a_ssem,
    a_rsem,
    b_ssem,
    b_rsem,
    ga_ssem,
    ga_rsem,
    gb_ssem,
    gb_rsem,
    ws_ssem,
    ws_rsem,
    wb_ssem,
    wb_rsem,
    n_ssem,
    n_rsem,
):
    r, c = lax.axis_index("row"), lax.axis_index("col")
    Z, N = C // 2, R * C
    z, q = c // 2, c % 2
    me = r * C + c
    T = a_ref.shape[1]
    K, H = a_ref.shape[2], a_ref.shape[3]
    KH = K // 2
    J = R * T

    def where(d):
        return (d // C, d % C)

    col_peers = [(s, lax.rem(c + s, C)) for s in range(1, C)]
    row_peers = [lax.rem(r + s, R) for s in range(1, R)]

    barrier = pltpu.get_barrier_semaphore()
    if fused:
        for s in range(1, N):
            pl.semaphore_signal(barrier, 1, device_id=where(lax.rem(me + s, N)), device_id_type=MESH)
        expected = N - 1
    else:
        for _, cc in col_peers:
            pl.semaphore_signal(barrier, 1, device_id=(r, cc), device_id_type=MESH)
        for rr in row_peers:
            for p in range(2):
                pl.semaphore_signal(barrier, 1, device_id=(rr, z * 2 + p), device_id_type=MESH)
        expected = C - 1 + 2 * (R - 1)

    loads = []
    for n, (src, dst) in enumerate(
        (
            (a_hbm, a_ref),
            (b_hbm, b_ref),
            (dt_hbm, dt_ref),
            (z_hbm, z_ref),
            (gain_hbm, gain_ref),
            (bias_hbm, bias_ref),
            (w_hbm, w_ref),
        )
    ):
        load = pltpu.make_async_copy(src, dst, in_sem.at[n])
        load.start()
        loads.append(load)
    for load in loads[:3]:
        load.wait()
    pl.semaphore_wait(barrier, expected)

    def remote(src, dst, ssem, rsem, dev):
        return pltpu.make_async_remote_copy(
            src_ref=src, dst_ref=dst, send_sem=ssem, recv_sem=rsem, device_id=dev, device_id_type=MESH
        )

    other = z * 2 + (1 - q)

    def half(p):
        return pl.ds(p * KH if isinstance(p, int) else pl.multiple_of(p * KH, KH), KH)

    sends = []

    def push(copy):
        copy.start()
        sends.append(copy)

    push(remote(dt_ref, dt_other, dt_sem.at[0], dt_sem.at[1], (r, other)))
    push(remote(b_ref.at[0, :, half(1 - q), :], b_all.at[q, pl.ds(r * T, T)], b_ssem.at[r, 1 - q], b_rsem.at[r, q], (r, other)))
    for rr in row_peers:
        for p in range(2):
            push(remote(b_ref.at[0, :, half(p), :], b_all.at[q, pl.ds(r * T, T)], b_ssem.at[rr, p], b_rsem.at[r, q], (rr, z * 2 + p)))
    for s in range(1, Z):
        zz = lax.rem(z + s, Z)
        for p in range(2):
            push(remote(a_ref.at[0, :, half(p), :], a_all.at[pl.ds(c * T, T)], a_ssem.at[zz * 2 + p], a_rsem.at[c], (r, zz * 2 + p)))
    push(remote(a_ref.at[0, :, half(1 - q), :], a_all.at[pl.ds(c * T, T)], a_ssem.at[other], a_rsem.at[c], (r, other)))

    for t in range(T):
        a_all[c * T + t] = a_ref[0, t, half(q), :]
        b_all[q, r * T + t] = b_ref[0, t, half(q), :]
    dtf[q] = dt_ref[...].reshape(C * T, J, H).astype(F32)

    for load in loads[3:]:
        load.wait()
    pair = z_ref[...].reshape(T * K, H).astype(F32)
    average = jnp.mean(pair, axis=-1, keepdims=True)
    centred = pair - average
    variance = jnp.mean(centred * centred, axis=-1, keepdims=True)
    inv_std = lax.rsqrt(variance + 1e-05)
    xhat = centred * inv_std
    normed32 = xhat * gain_ref[...] + bias_ref[...]
    normed = normed32.astype(BF16)
    normt_ref[...] = jnp.transpose(normed32).astype(BF16)
    xhat_ref[...] = xhat
    inv_ref[...] = jnp.broadcast_to(inv_std, inv_ref.shape)
    for m in range(2):
        gate = jax.nn.sigmoid(jnp.dot(normed, w_ref[2 * m], preferred_element_type=F32))
        value = jnp.dot(normed, w_ref[2 * m + 1], preferred_element_type=F32)
        coef[2 * m] = value * gate * (1.0 - gate)
        coef[2 * m + 1] = gate

    remote(dt_ref, dt_other, dt_sem.at[0], dt_sem.at[1], (r, other)).wait_recv()
    dtf[1 - q] = dt_other[...].reshape(C * T, J, H).astype(F32)

    def b_wait(rr, p):
        remote(b_all.at[p, pl.ds(rr * T, T)], b_all.at[p, pl.ds(rr * T, T)], b_ssem.at[rr, p], b_rsem.at[rr, p], (r, other)).wait_recv()

    b_wait(r, 1 - q)
    for rr in row_peers:
        for p in range(2):
            b_wait(rr, p)

    zero = jnp.zeros((KH, H), F32)
    for s in list(range(1, Z)) + [0]:
        zz = lax.rem(z + s, Z)
        acc = (zero,) * (2 * T)
        for core in range(2):

            def step(j, acc, core=core, zz=zz):
                right = b_all[core, j].astype(F32)
                return tuple(
                    acc[n] + dtf[core, zz * 2 * T + n, pl.ds(j, 1), :] * right for n in range(2 * T)
                )

            acc = lax.fori_loop(0, J, step, acc, unroll=4)
        if s:
            for p in range(2):
                for t in range(T):
                    ga_send[s, p, t] = acc[p * T + t].astype(BF16)
                push(remote(ga_send.at[s, p], ga_all.at[z, q], ga_ssem.at[s, p], ga_rsem.at[z, q], (r, zz * 2 + p)))
        else:
            for t in range(T):
                keep = jnp.where(q == 0, acc[t], acc[T + t])
                give = jnp.where(q == 0, acc[T + t], acc[t])
                ga_send[0, 0, t] = give.astype(BF16)
                ga_all[z, q, t] = keep.astype(BF16)
            push(remote(ga_send.at[0, 0], ga_all.at[z, q], ga_ssem.at[0, 0], ga_rsem.at[z, q], (r, other)))

    def a_wait(cc):
        remote(a_all.at[pl.ds(cc * T, T)], a_all.at[pl.ds(cc * T, T)], a_ssem.at[cc], a_rsem.at[cc], (r, other)).wait_recv()

    for _, cc in col_peers:
        a_wait(cc)
    for s in list(range(1, R)) + [0]:
        rr = lax.rem(r + s, R)

        def step(i, acc, rr=rr):
            left = a_all[i].astype(F32)
            return tuple(
                acc[n] + dtf[n // T, i, pl.ds(rr * T + n % T, 1), :] * left for n in range(2 * T)
            )

        acc = lax.fori_loop(0, C * T, step, (zero,) * (2 * T), unroll=4)
        if s:
            for p in range(2):
                for t in range(T):
                    gb_send[s, p, t] = acc[p * T + t].astype(BF16)
                push(remote(gb_send.at[s, p], gb_all.at[r, q], gb_ssem.at[s, p], gb_rsem.at[r, q], (rr, z * 2 + p)))
        else:
            for t in range(T):
                keep = jnp.where(q == 0, acc[t], acc[T + t])
                give = jnp.where(q == 0, acc[T + t], acc[t])
                gb_send[0, 0, t] = give.astype(BF16)
                gb_all[r, q, t] = keep.astype(BF16)
            push(remote(gb_send.at[0, 0], gb_all.at[r, q], gb_ssem.at[0, 0], gb_rsem.at[r, q], (r, other)))

    def total(buf, count):
        rows = []
        for t in range(T):
            for p in range(2):
                acc = buf[0, p, t].astype(F32)
                for n in range(1, count):
                    acc = acc + buf[n, p, t].astype(F32)
                rows.append(acc)
        return jnp.concatenate(rows, axis=0)

    def slot_wait(buf, sem, n, p):
        remote(buf.at[n, p], buf.at[n, p], dt_sem.at[0], sem.at[n, p], (r, other)).wait_recv()

    chunk = 2 * H // N if fused else 0
    normt = normt_ref[...]

    def weight_part(m, g):
        part = jnp.dot(normt, g, preferred_element_type=F32)
        if fused:
            per = part.shape[0] // chunk
            at = (m % 2) * per
            wsend[m // 2, at : at + per] = part.astype(BF16).reshape(per, chunk, H)
        else:
            wgrad_ref[m] = part

    def spread(side):
        for s in range(1, N):
            d = lax.rem(me + s, N)
            push(remote(wsend.at[side, d], wrecv.at[side, me], ws_ssem.at[side, s], ws_rsem.at[side, me], where(d)))
        wrecv[side, me] = wsend[side, me]

    def collect(side):
        for s in range(1, N):
            d = lax.rem(me + s, N)
            remote(wrecv.at[side, d], wrecv.at[side, d], ws_ssem.at[side, s], ws_rsem.at[side, d], where(d)).wait_recv()
        acc = wrecv[side, 0].astype(F32)
        for n in range(1, N):
            acc = acc + wrecv[side, n].astype(F32)
        wback[side, me] = acc.astype(BF16)
        for s in range(1, N):
            d = lax.rem(me + s, N)
            push(remote(wback.at[side, me], wback.at[side, me], wb_ssem.at[side, s], wb_rsem.at[side, me], where(d)))

    def dn_part(m, g):
        return lax.dot_general(g, w_ref[m], (((1,), (1,)), ((), ())), preferred_element_type=F32)

    for s in list(range(1, Z)):
        zz = lax.rem(z + s, Z)
        for p in range(2):
            slot_wait(ga_all, ga_rsem, zz, p)
    slot_wait(ga_all, ga_rsem, z, 1 - q)
    left_grad = total(ga_all, Z)
    g = [(left_grad * coef[m]).astype(BF16) for m in range(2)]
    weight_part(0, g[0])
    weight_part(1, g[1])
    if fused:
        spread(0)
    dn = dn_part(0, g[0]) + dn_part(1, g[1])

    for s in list(range(1, R)):
        rr = lax.rem(r + s, R)
        for p in range(2):
            slot_wait(gb_all, gb_rsem, rr, p)
    slot_wait(gb_all, gb_rsem, r, 1 - q)
    right_grad = total(gb_all, R)
    g = [(right_grad * coef[m]).astype(BF16) for m in range(2, 4)]
    weight_part(2, g[0])
    weight_part(3, g[1])
    if fused:
        spread(1)
    dn = dn + dn_part(2, g[0]) + dn_part(3, g[1])

    xhat = xhat_ref[...]
    norm_part = jnp.concatenate(
        [jnp.sum(dn * xhat, axis=0, keepdims=True), jnp.sum(dn, axis=0, keepdims=True)], axis=0
    )
    if fused:
        nrecv[me] = norm_part
        for s in range(1, N):
            d = lax.rem(me + s, N)
            push(remote(nrecv.at[me], nrecv.at[me], n_ssem.at[s], n_rsem.at[me], where(d)))
    else:
        norm_ref[...] = norm_part
    dh = dn * gain_ref[...]
    grad = inv_ref[...] * (
        dh
        - jnp.mean(dh, axis=-1, keepdims=True)
        - xhat * jnp.mean(dh * xhat, axis=-1, keepdims=True)
    )
    pair_ref[...] = grad.astype(BF16).reshape(pair_ref.shape)

    if fused:
        collect(0)
        collect(1)
        for s in range(1, N):
            d = lax.rem(me + s, N)
            remote(nrecv.at[d], nrecv.at[d], n_ssem.at[s], n_rsem.at[d], where(d)).wait_recv()
        acc = nrecv[0]
        for n in range(1, N):
            acc = acc + nrecv[n]
        norm_ref[...] = acc
        for s in range(1, N):
            d = lax.rem(me + s, N)
            for side in range(2):
                remote(wback.at[side, d], wback.at[side, d], wb_ssem.at[side, s], wb_rsem.at[side, d], where(d)).wait_recv()
        wgrad_ref[...] = wback[...].reshape(wgrad_ref.shape)
    for copy in sends:
        copy.wait_send()


def finish(pair_ref, wgrad_ref, norm_ref, pair_out, wgrad_out, norm_out, wide, sem):
    copies = [
        pltpu.make_async_copy(pair_ref, pair_out, sem.at[0]),
        pltpu.make_async_copy(norm_ref, norm_out, sem.at[1]),
    ]
    for copy in copies:
        copy.start()
    for m in range(wide.shape[0]):
        wide[m] = wgrad_ref[m].astype(F32)
        copies.append(pltpu.make_async_copy(wide.at[m], wgrad_out.at[m], sem.at[2 + m]))
        copies[-1].start()
    for copy in copies:
        copy.wait()


def on_device(R, C, z, dt, a, b, gain, bias, w):
    _, T, K, H = a.shape
    J = dt.shape[2]
    KH, Z, N = K // 2, C // 2, R * C
    fused = (4 * H) % (16 * N) == 0
    M = N if fused else 1
    chunk = 2 * H // N if fused else 8
    V = pltpu.VMEM
    D = pltpu.SemaphoreType.DMA
    anyspace = pl.BlockSpec(memory_space=pl.ANY)
    vspace = pl.BlockSpec(memory_space=pltpu.VMEM)
    pair, wgrad, norm = pl.pallas_call(
        functools.partial(kernel, R, C, fused),
        out_shape=(
            pltpu.VMEM(z.shape, BF16),
            pltpu.VMEM(w.shape, BF16 if fused else F32),
            pltpu.VMEM((2, z.shape[3]), F32),
        ),
        in_specs=[anyspace] * 7,
        out_specs=(vspace,) * 3,
        scratch_shapes=[
            V(z.shape, BF16),
            V(dt.shape, BF16),
            V(a.shape, BF16),
            V(b.shape, BF16),
            V((1, H), F32),
            V((1, H), F32),
            V(w.shape, BF16),
            V(dt.shape, BF16),
            V((2, C * T, J, H), F32),
            V((C * T, KH, H), BF16),
            V((2, J, KH, H), BF16),
            V((Z, 2, T, KH, H), BF16),
            V((R, 2, T, KH, H), BF16),
            V((Z, 2, T, KH, H), BF16),
            V((R, 2, T, KH, H), BF16),
            V((4, T * K, H), F32),
            V((T * K, H), F32),
            V((H, T * K), BF16),
            V((T * K, H), F32),
            V((2, M, chunk, H), BF16),
            V((2, M, chunk, H), BF16),
            V((2, M, chunk, H), BF16),
            V((M, 2, H), F32),
            D((7,)),
            D((2,)),
            D((C,)),
            D((C,)),
            D((R, 2)),
            D((R, 2)),
            D((Z, 2)),
            D((Z, 2)),
            D((R, 2)),
            D((R, 2)),
            D((2, M)),
            D((2, M)),
            D((2, M)),
            D((2, M)),
            D((M,)),
            D((M,)),
        ],
        compiler_params=pltpu.CompilerParams(
            collective_id=0, has_side_effects=True, vmem_limit_bytes=56 * 1024 * 1024
        ),
    )(z, dt, a, b, gain.reshape(1, -1), bias.reshape(1, -1), w)
    if not fused:
        wgrad, norm = lax.psum((wgrad, norm), ("row", "col"))
    return pl.pallas_call(
        finish,
        out_shape=(
            jax.ShapeDtypeStruct(z.shape, BF16),
            jax.ShapeDtypeStruct(w.shape, F32),
            jax.ShapeDtypeStruct(norm.shape, F32),
        ),
        in_specs=[vspace] * 3,
        out_specs=(anyspace,) * 3,
        scratch_shapes=[V(w.shape, F32), D((2 + w.shape[0],))],
        compiler_params=pltpu.CompilerParams(vmem_limit_bytes=4 * 1024 * 1024),
    )(pair, wgrad, norm)


def solution(mesh):
    R, C = mesh.shape["row"], mesh.shape["col"]
    return jax.shard_map(
        functools.partial(on_device, R, C),
        mesh=mesh,
        in_specs=(
            P("col", "row", None, None),
            P(None, "row", "col", None),
            P("col", "row", None, None),
            P("col", "row", None, None),
            P(),
            P(),
            P(),
        ),
        out_specs=(P("col", "row", None, None), P(), P()),
        check_vma=False,
    )
```

```python
import functools

import jax
import jax.numpy as jnp
from jax import lax
from jax.experimental import pallas as pl
from jax.experimental.pallas import tpu as pltpu
from jax.sharding import PartitionSpec as P

MESH = pl.DeviceIdType.MESH
F32 = jnp.float32
BF16 = jnp.bfloat16


def kernel(
    R,
    C,
    fused,
    z_hbm,
    dt_hbm,
    a_hbm,
    b_hbm,
    gain_hbm,
    bias_hbm,
    w_hbm,
    pair_ref,
    wgrad_ref,
    norm_ref,
    z_ref,
    dt_ref,
    a_ref,
    b_ref,
    gain_ref,
    bias_ref,
    w_ref,
    dt_other,
    dtf,
    a_all,
    b_all,
    ga_send,
    gb_send,
    ga_all,
    gb_all,
    coef,
    xhat_ref,
    normt_ref,
    inv_ref,
    wsend,
    wrecv,
    wback,
    nrecv,
    in_sem,
    dt_sem,
    a_ssem,
    a_rsem,
    b_ssem,
    b_rsem,
    ga_ssem,
    ga_rsem,
    gb_ssem,
    gb_rsem,
    ws_ssem,
    ws_rsem,
    wb_ssem,
    wb_rsem,
    n_ssem,
    n_rsem,
):
    r, c = lax.axis_index("row"), lax.axis_index("col")
    Z, N = C // 2, R * C
    z, q = c // 2, c % 2
    me = r * C + c
    T = a_ref.shape[1]
    K, H = a_ref.shape[2], a_ref.shape[3]
    KH = K // 2
    J = R * T

    def where(d):
        return (d // C, d % C)

    col_peers = [(s, lax.rem(c + s, C)) for s in range(1, C)]
    row_peers = [lax.rem(r + s, R) for s in range(1, R)]

    barrier = pltpu.get_barrier_semaphore()
    for _, cc in col_peers:
        pl.semaphore_signal(barrier, 1, device_id=(r, cc), device_id_type=MESH)
    for rr in row_peers:
        for p in range(2):
            pl.semaphore_signal(barrier, 1, device_id=(rr, z * 2 + p), device_id_type=MESH)
    expected = C - 1 + 2 * (R - 1)

    loads = []
    for n, (src, dst) in enumerate(
        (
            (a_hbm, a_ref),
            (b_hbm, b_ref),
            (dt_hbm, dt_ref),
            (z_hbm, z_ref),
            (gain_hbm, gain_ref),
            (bias_hbm, bias_ref),
            (w_hbm, w_ref),
        )
    ):
        load = pltpu.make_async_copy(src, dst, in_sem.at[n])
        load.start()
        loads.append(load)
    for load in loads[:3]:
        load.wait()
    pl.semaphore_wait(barrier, expected)

    def remote(src, dst, ssem, rsem, dev):
        return pltpu.make_async_remote_copy(
            src_ref=src, dst_ref=dst, send_sem=ssem, recv_sem=rsem, device_id=dev, device_id_type=MESH
        )

    other = z * 2 + (1 - q)

    def half(p):
        return pl.ds(p * KH if isinstance(p, int) else pl.multiple_of(p * KH, KH), KH)

    sends = []

    def push(copy):
        copy.start()
        sends.append(copy)

    push(remote(dt_ref, dt_other, dt_sem.at[0], dt_sem.at[1], (r, other)))
    push(remote(b_ref.at[0, :, half(1 - q), :], b_all.at[q, pl.ds(r * T, T)], b_ssem.at[r, 1 - q], b_rsem.at[r, q], (r, other)))
    for rr in row_peers:
        for p in range(2):
            push(remote(b_ref.at[0, :, half(p), :], b_all.at[q, pl.ds(r * T, T)], b_ssem.at[rr, p], b_rsem.at[r, q], (rr, z * 2 + p)))
    for s in range(1, Z):
        zz = lax.rem(z + s, Z)
        for p in range(2):
            push(remote(a_ref.at[0, :, half(p), :], a_all.at[pl.ds(c * T, T)], a_ssem.at[zz * 2 + p], a_rsem.at[c], (r, zz * 2 + p)))
    push(remote(a_ref.at[0, :, half(1 - q), :], a_all.at[pl.ds(c * T, T)], a_ssem.at[other], a_rsem.at[c], (r, other)))

    for t in range(T):
        a_all[c * T + t] = a_ref[0, t, half(q), :]
        b_all[q, r * T + t] = b_ref[0, t, half(q), :]
    dtf[q] = dt_ref[...].reshape(C * T, J, H).astype(F32)

    for load in loads[3:]:
        load.wait()
    pair = z_ref[...].reshape(T * K, H).astype(F32)
    average = jnp.mean(pair, axis=-1, keepdims=True)
    centred = pair - average
    variance = jnp.mean(centred * centred, axis=-1, keepdims=True)
    inv_std = lax.rsqrt(variance + 1e-05)
    xhat = centred * inv_std
    normed32 = xhat * gain_ref[...] + bias_ref[...]
    normed = normed32.astype(BF16)
    normt_ref[...] = jnp.transpose(normed32).astype(BF16)
    xhat_ref[...] = xhat
    inv_ref[...] = jnp.broadcast_to(inv_std, inv_ref.shape)
    for m in range(2):
        gate = jax.nn.sigmoid(jnp.dot(normed, w_ref[2 * m], preferred_element_type=F32))
        value = jnp.dot(normed, w_ref[2 * m + 1], preferred_element_type=F32)
        coef[2 * m] = value * gate * (1.0 - gate)
        coef[2 * m + 1] = gate

    remote(dt_ref, dt_other, dt_sem.at[0], dt_sem.at[1], (r, other)).wait_recv()
    dtf[1 - q] = dt_other[...].reshape(C * T, J, H).astype(F32)

    def b_wait(rr, p):
        remote(b_all.at[p, pl.ds(rr * T, T)], b_all.at[p, pl.ds(rr * T, T)], b_ssem.at[rr, p], b_rsem.at[rr, p], (r, other)).wait_recv()

    b_wait(r, 1 - q)
    for rr in row_peers:
        for p in range(2):
            b_wait(rr, p)

    zero = jnp.zeros((KH, H), F32)
    for s in list(range(1, Z)) + [0]:
        zz = lax.rem(z + s, Z)
        acc = (zero,) * (2 * T)
        for core in range(2):

            def step(j, acc, core=core, zz=zz):
                right = b_all[core, j].astype(F32)
                return tuple(
                    acc[n] + dtf[core, zz * 2 * T + n, pl.ds(j, 1), :] * right for n in range(2 * T)
                )

            acc = lax.fori_loop(0, J, step, acc, unroll=4)
        if s:
            for p in range(2):
                for t in range(T):
                    ga_send[s, p, t] = acc[p * T + t].astype(BF16)
                push(remote(ga_send.at[s, p], ga_all.at[z, q], ga_ssem.at[s, p], ga_rsem.at[z, q], (r, zz * 2 + p)))
        else:
            for t in range(T):
                keep = jnp.where(q == 0, acc[t], acc[T + t])
                give = jnp.where(q == 0, acc[T + t], acc[t])
                ga_send[0, 0, t] = give.astype(BF16)
                ga_all[z, q, t] = keep.astype(BF16)
            push(remote(ga_send.at[0, 0], ga_all.at[z, q], ga_ssem.at[0, 0], ga_rsem.at[z, q], (r, other)))

    def a_wait(cc):
        remote(a_all.at[pl.ds(cc * T, T)], a_all.at[pl.ds(cc * T, T)], a_ssem.at[cc], a_rsem.at[cc], (r, other)).wait_recv()

    for _, cc in col_peers:
        a_wait(cc)
    for s in list(range(1, R)) + [0]:
        rr = lax.rem(r + s, R)

        def step(i, acc, rr=rr):
            left = a_all[i].astype(F32)
            return tuple(
                acc[n] + dtf[n // T, i, pl.ds(rr * T + n % T, 1), :] * left for n in range(2 * T)
            )

        acc = lax.fori_loop(0, C * T, step, (zero,) * (2 * T), unroll=4)
        if s:
            for p in range(2):
                for t in range(T):
                    gb_send[s, p, t] = acc[p * T + t].astype(BF16)
                push(remote(gb_send.at[s, p], gb_all.at[r, q], gb_ssem.at[s, p], gb_rsem.at[r, q], (rr, z * 2 + p)))
        else:
            for t in range(T):
                keep = jnp.where(q == 0, acc[t], acc[T + t])
                give = jnp.where(q == 0, acc[T + t], acc[t])
                gb_send[0, 0, t] = give.astype(BF16)
                gb_all[r, q, t] = keep.astype(BF16)
            push(remote(gb_send.at[0, 0], gb_all.at[r, q], gb_ssem.at[0, 0], gb_rsem.at[r, q], (r, other)))

    def total(buf, count):
        rows = []
        for t in range(T):
            for p in range(2):
                acc = buf[0, p, t].astype(F32)
                for n in range(1, count):
                    acc = acc + buf[n, p, t].astype(F32)
                rows.append(acc)
        return jnp.concatenate(rows, axis=0)

    def slot_wait(buf, sem, n, p):
        remote(buf.at[n, p], buf.at[n, p], dt_sem.at[0], sem.at[n, p], (r, other)).wait_recv()

    O = 2 * R
    chunk = 2 * H // O if fused else 0
    mid = Z // 2
    nearest = r * 2 + jnp.where(z >= mid, 1, 0)
    is_owner = (q == 1) & ((z == mid - 1) | (z == mid))

    def owner_device(o):
        return (o // 2, (mid - 1 + o % 2) * 2 + 1)

    def await_all(buf, count, ssem, rsem):
        part = buf.at[pl.ds(0, count)]
        return remote(part, part, ssem, rsem, (r, other))

    normt = normt_ref[...]

    def weight_part(m, g):
        part = jnp.dot(normt, g, preferred_element_type=F32)
        if fused:
            per = part.shape[0] // chunk
            at = (m % 2) * per
            wsend[m // 2, at : at + per] = part.astype(BF16).reshape(per, chunk, H)
        else:
            wgrad_ref[m] = part

    def spread(side):
        for s in range(1, O):
            o = lax.rem(nearest + s, O)
            remote(wsend.at[side, o], wrecv.at[side, me], ws_ssem.at[side], ws_rsem.at[side], owner_device(o)).start()

        @pl.when(is_owner)
        def _():
            wrecv[side, me] = wsend[side, nearest]

        @pl.when(jnp.logical_not(is_owner))
        def _():
            remote(wsend.at[side, nearest], wrecv.at[side, me], ws_ssem.at[side], ws_rsem.at[side], owner_device(nearest)).start()

    def collect(side):
        await_all(wrecv.at[side], N - 1, ws_ssem.at[side], ws_rsem.at[side]).wait_recv()
        acc = wrecv[side, 0].astype(F32)
        for n in range(1, N):
            acc = acc + wrecv[side, n].astype(F32)
        wback[side, nearest] = acc.astype(BF16)
        for s in range(1, N):
            d = lax.rem(me + s, N)
            remote(wback.at[side, nearest], wback.at[side, nearest], wb_ssem.at[side], wb_rsem.at[side], where(d)).start()

    def dn_part(m, g):
        return lax.dot_general(g, w_ref[m], (((1,), (1,)), ((), ())), preferred_element_type=F32)

    for s in list(range(1, Z)):
        zz = lax.rem(z + s, Z)
        for p in range(2):
            slot_wait(ga_all, ga_rsem, zz, p)
    slot_wait(ga_all, ga_rsem, z, 1 - q)
    left_grad = total(ga_all, Z)
    g = [(left_grad * coef[m]).astype(BF16) for m in range(2)]
    weight_part(0, g[0])
    weight_part(1, g[1])
    if fused:
        spread(0)
    dn = dn_part(0, g[0]) + dn_part(1, g[1])

    for s in list(range(1, R)):
        rr = lax.rem(r + s, R)
        for p in range(2):
            slot_wait(gb_all, gb_rsem, rr, p)
    slot_wait(gb_all, gb_rsem, r, 1 - q)
    right_grad = total(gb_all, R)
    g = [(right_grad * coef[m]).astype(BF16) for m in range(2, 4)]
    weight_part(2, g[0])
    weight_part(3, g[1])
    if fused:
        spread(1)
    dn = dn + dn_part(2, g[0]) + dn_part(3, g[1])

    xhat = xhat_ref[...]
    norm_part = jnp.concatenate(
        [jnp.sum(dn * xhat, axis=0, keepdims=True), jnp.sum(dn, axis=0, keepdims=True)], axis=0
    )
    if fused:
        nrecv[me] = norm_part
        for s in range(1, N):
            d = lax.rem(me + s, N)
            remote(nrecv.at[me], nrecv.at[me], n_ssem.at[0], n_rsem.at[0], where(d)).start()
    else:
        norm_ref[...] = norm_part
    dh = dn * gain_ref[...]
    grad = inv_ref[...] * (
        dh
        - jnp.mean(dh, axis=-1, keepdims=True)
        - xhat * jnp.mean(dh * xhat, axis=-1, keepdims=True)
    )
    pair_ref[...] = grad.astype(BF16).reshape(pair_ref.shape)

    if fused:

        @pl.when(is_owner)
        def _():
            collect(0)
            collect(1)

        await_all(nrecv, N - 1, n_ssem.at[0], n_rsem.at[0]).wait()
        acc = nrecv[0]
        for n in range(1, N):
            acc = acc + nrecv[n]
        norm_ref[...] = acc

        @pl.when(is_owner)
        def _():
            for side in range(2):
                await_all(wback.at[side], O - 1, ws_ssem.at[side], wb_rsem.at[side]).wait()
                await_all(wrecv.at[side], N - 1, wb_ssem.at[side], wb_rsem.at[side]).wait_send()

        @pl.when(jnp.logical_not(is_owner))
        def _():
            for side in range(2):
                await_all(wback.at[side], O, ws_ssem.at[side], wb_rsem.at[side]).wait()

        wgrad_ref[...] = wback[...].reshape(wgrad_ref.shape)
    for copy in sends:
        copy.wait_send()


def finish(pair_ref, wgrad_ref, norm_ref, pair_out, wgrad_out, norm_out, wide, sem):
    copies = [
        pltpu.make_async_copy(pair_ref, pair_out, sem.at[0]),
        pltpu.make_async_copy(norm_ref, norm_out, sem.at[1]),
    ]
    for copy in copies:
        copy.start()
    for m in range(wide.shape[0]):
        wide[m] = wgrad_ref[m].astype(F32)
        copies.append(pltpu.make_async_copy(wide.at[m], wgrad_out.at[m], sem.at[2 + m]))
        copies[-1].start()
    for copy in copies:
        copy.wait()


def on_device(R, C, z, dt, a, b, gain, bias, w):
    _, T, K, H = a.shape
    J = dt.shape[2]
    KH, Z, N = K // 2, C // 2, R * C
    fused = (4 * H) % (16 * N) == 0
    M, O = (N, 2 * R) if fused else (1, 1)
    chunk = 2 * H // O if fused else 8
    V = pltpu.VMEM
    D = pltpu.SemaphoreType.DMA
    anyspace = pl.BlockSpec(memory_space=pl.ANY)
    vspace = pl.BlockSpec(memory_space=pltpu.VMEM)
    pair, wgrad, norm = pl.pallas_call(
        functools.partial(kernel, R, C, fused),
        out_shape=(
            pltpu.VMEM(z.shape, BF16),
            pltpu.VMEM(w.shape, BF16 if fused else F32),
            pltpu.VMEM((2, z.shape[3]), F32),
        ),
        in_specs=[anyspace] * 7,
        out_specs=(vspace,) * 3,
        scratch_shapes=[
            V(z.shape, BF16),
            V(dt.shape, BF16),
            V(a.shape, BF16),
            V(b.shape, BF16),
            V((1, H), F32),
            V((1, H), F32),
            V(w.shape, BF16),
            V(dt.shape, BF16),
            V((2, C * T, J, H), F32),
            V((C * T, KH, H), BF16),
            V((2, J, KH, H), BF16),
            V((Z, 2, T, KH, H), BF16),
            V((R, 2, T, KH, H), BF16),
            V((Z, 2, T, KH, H), BF16),
            V((R, 2, T, KH, H), BF16),
            V((4, T * K, H), F32),
            V((T * K, H), F32),
            V((H, T * K), BF16),
            V((T * K, H), F32),
            V((2, O, chunk, H), BF16),
            V((2, M, chunk, H), BF16),
            V((2, O, chunk, H), BF16),
            V((M, 2, H), F32),
            D((7,)),
            D((2,)),
            D((C,)),
            D((C,)),
            D((R, 2)),
            D((R, 2)),
            D((Z, 2)),
            D((Z, 2)),
            D((R, 2)),
            D((R, 2)),
            D((2,)),
            D((2,)),
            D((2,)),
            D((2,)),
            D((1,)),
            D((1,)),
        ],
        compiler_params=pltpu.CompilerParams(
            collective_id=0, has_side_effects=True, vmem_limit_bytes=56 * 1024 * 1024
        ),
    )(z, dt, a, b, gain.reshape(1, -1), bias.reshape(1, -1), w)
    if not fused:
        wgrad, norm = lax.psum((wgrad, norm), ("row", "col"))
    return pl.pallas_call(
        finish,
        out_shape=(
            jax.ShapeDtypeStruct(z.shape, BF16),
            jax.ShapeDtypeStruct(w.shape, F32),
            jax.ShapeDtypeStruct(norm.shape, F32),
        ),
        in_specs=[vspace] * 3,
        out_specs=(anyspace,) * 3,
        scratch_shapes=[V(w.shape, F32), D((2 + w.shape[0],))],
        compiler_params=pltpu.CompilerParams(vmem_limit_bytes=4 * 1024 * 1024),
    )(pair, wgrad, norm)


def solution(mesh):
    R, C = mesh.shape["row"], mesh.shape["col"]
    return jax.shard_map(
        functools.partial(on_device, R, C),
        mesh=mesh,
        in_specs=(
            P("col", "row", None, None),
            P(None, "row", "col", None),
            P("col", "row", None, None),
            P("col", "row", None, None),
            P(),
            P(),
            P(),
        ),
        out_specs=(P("col", "row", None, None), P(), P()),
        check_vma=False,
    )
```

```python
import functools

import jax
import jax.numpy as jnp
from jax import lax
from jax.experimental import pallas as pl
from jax.experimental.pallas import tpu as pltpu
from jax.sharding import PartitionSpec as P

MESH = pl.DeviceIdType.MESH
F32 = jnp.float32
BF16 = jnp.bfloat16


def kernel(
    R,
    C,
    fused,
    z_hbm,
    dt_hbm,
    a_hbm,
    b_hbm,
    gain_hbm,
    bias_hbm,
    w_hbm,
    pair_ref,
    wgrad_ref,
    norm_ref,
    z_ref,
    dt_ref,
    a_ref,
    b_ref,
    gain_ref,
    bias_ref,
    w_ref,
    dt_other,
    dtf,
    a_all,
    b_all,
    ga_send,
    gb_send,
    ga_all,
    gb_all,
    coef,
    xhat_ref,
    normt_ref,
    inv_ref,
    wsend,
    wrecv,
    wback,
    nrecv,
    in_sem,
    dt_sem,
    a_ssem,
    a_rsem,
    b_ssem,
    b_rsem,
    ga_ssem,
    ga_rsem,
    gb_ssem,
    gb_rsem,
    ws_ssem,
    ws_rsem,
    wb_ssem,
    wb_rsem,
    n_ssem,
    n_rsem,
):
    r, c = lax.axis_index("row"), lax.axis_index("col")
    Z, N = C // 2, R * C
    z, q = c // 2, c % 2
    me = r * C + c
    T = a_ref.shape[1]
    K, H = a_ref.shape[2], a_ref.shape[3]
    KH = K // 2
    J = R * T

    def where(d):
        return (d // C, d % C)

    col_peers = [(s, lax.rem(c + s, C)) for s in range(1, C)]
    row_peers = [lax.rem(r + s, R) for s in range(1, R)]

    barrier = pltpu.get_barrier_semaphore()
    for _, cc in col_peers:
        pl.semaphore_signal(barrier, 1, device_id=(r, cc), device_id_type=MESH)
    for rr in row_peers:
        for p in range(2):
            pl.semaphore_signal(barrier, 1, device_id=(rr, z * 2 + p), device_id_type=MESH)
    expected = C - 1 + 2 * (R - 1)

    loads = []
    for n, (src, dst) in enumerate(
        (
            (a_hbm, a_ref),
            (b_hbm, b_ref),
            (dt_hbm, dt_ref),
            (z_hbm, z_ref),
            (gain_hbm, gain_ref),
            (bias_hbm, bias_ref),
            (w_hbm, w_ref),
        )
    ):
        load = pltpu.make_async_copy(src, dst, in_sem.at[n])
        load.start()
        loads.append(load)
    for load in loads[:3]:
        load.wait()
    pl.semaphore_wait(barrier, expected)

    def remote(src, dst, ssem, rsem, dev):
        return pltpu.make_async_remote_copy(
            src_ref=src, dst_ref=dst, send_sem=ssem, recv_sem=rsem, device_id=dev, device_id_type=MESH
        )

    other = z * 2 + (1 - q)

    def half(p):
        return pl.ds(p * KH if isinstance(p, int) else pl.multiple_of(p * KH, KH), KH)

    sends = []

    def push(copy):
        copy.start()
        sends.append(copy)

    for rr in row_peers:
        for p in range(2):
            push(remote(b_ref.at[0, :, half(p), :], b_all.at[q, pl.ds(r * T, T)], b_ssem.at[rr, p], b_rsem.at[r, q], (rr, z * 2 + p)))
    push(remote(b_ref.at[0, :, half(1 - q), :], b_all.at[q, pl.ds(r * T, T)], b_ssem.at[r, 1 - q], b_rsem.at[r, q], (r, other)))
    push(remote(dt_ref, dt_other, dt_sem.at[0], dt_sem.at[1], (r, other)))
    for s in range(1, Z):
        zz = lax.rem(z + s, Z)
        for p in range(2):
            push(remote(a_ref.at[0, :, half(p), :], a_all.at[pl.ds(c * T, T)], a_ssem.at[zz * 2 + p], a_rsem.at[c], (r, zz * 2 + p)))
    push(remote(a_ref.at[0, :, half(1 - q), :], a_all.at[pl.ds(c * T, T)], a_ssem.at[other], a_rsem.at[c], (r, other)))

    for t in range(T):
        a_all[c * T + t] = a_ref[0, t, half(q), :]
        b_all[q, r * T + t] = b_ref[0, t, half(q), :]
    dtf[q] = dt_ref[...].reshape(C * T, J, H).astype(F32)

    for load in loads[3:]:
        load.wait()
    pair = z_ref[...].reshape(T * K, H).astype(F32)
    average = jnp.mean(pair, axis=-1, keepdims=True)
    centred = pair - average
    variance = jnp.mean(centred * centred, axis=-1, keepdims=True)
    inv_std = lax.rsqrt(variance + 1e-05)
    xhat = centred * inv_std
    normed32 = xhat * gain_ref[...] + bias_ref[...]
    normed = normed32.astype(BF16)
    normt_ref[...] = jnp.transpose(normed32).astype(BF16)
    xhat_ref[...] = xhat
    inv_ref[...] = jnp.broadcast_to(inv_std, inv_ref.shape)
    for m in range(2):
        gate = jax.nn.sigmoid(jnp.dot(normed, w_ref[2 * m], preferred_element_type=F32))
        value = jnp.dot(normed, w_ref[2 * m + 1], preferred_element_type=F32)
        coef[2 * m] = value * gate * (1.0 - gate)
        coef[2 * m + 1] = gate

    remote(dt_ref, dt_other, dt_sem.at[0], dt_sem.at[1], (r, other)).wait_recv()
    dtf[1 - q] = dt_other[...].reshape(C * T, J, H).astype(F32)

    def b_wait(rr, p):
        remote(b_all.at[p, pl.ds(rr * T, T)], b_all.at[p, pl.ds(rr * T, T)], b_ssem.at[rr, p], b_rsem.at[rr, p], (r, other)).wait_recv()

    b_wait(r, 1 - q)
    for rr in row_peers:
        for p in range(2):
            b_wait(rr, p)

    zero = jnp.zeros((KH, H), F32)
    for s in list(range(1, Z)) + [0]:
        zz = lax.rem(z + s, Z)
        acc = (zero,) * (2 * T)
        for core in range(2):

            def step(j, acc, core=core, zz=zz):
                right = b_all[core, j].astype(F32)
                return tuple(
                    acc[n] + dtf[core, zz * 2 * T + n, pl.ds(j, 1), :] * right for n in range(2 * T)
                )

            acc = lax.fori_loop(0, J, step, acc, unroll=4)
        if s:
            for p in range(2):
                for t in range(T):
                    ga_send[s, p, t] = acc[p * T + t].astype(BF16)
                push(remote(ga_send.at[s, p], ga_all.at[z, q], ga_ssem.at[s, p], ga_rsem.at[z, q], (r, zz * 2 + p)))
        else:
            for t in range(T):
                keep = jnp.where(q == 0, acc[t], acc[T + t])
                give = jnp.where(q == 0, acc[T + t], acc[t])
                ga_send[0, 0, t] = give.astype(BF16)
                ga_all[z, q, t] = keep.astype(BF16)
            push(remote(ga_send.at[0, 0], ga_all.at[z, q], ga_ssem.at[0, 0], ga_rsem.at[z, q], (r, other)))

    def a_wait(cc):
        remote(a_all.at[pl.ds(cc * T, T)], a_all.at[pl.ds(cc * T, T)], a_ssem.at[cc], a_rsem.at[cc], (r, other)).wait_recv()

    for _, cc in col_peers:
        a_wait(cc)
    for s in list(range(1, R)) + [0]:
        rr = lax.rem(r + s, R)

        def step(i, acc, rr=rr):
            left = a_all[i].astype(F32)
            return tuple(
                acc[n] + dtf[n // T, i, pl.ds(rr * T + n % T, 1), :] * left for n in range(2 * T)
            )

        acc = lax.fori_loop(0, C * T, step, (zero,) * (2 * T), unroll=4)
        if s:
            for p in range(2):
                for t in range(T):
                    gb_send[s, p, t] = acc[p * T + t].astype(BF16)
                push(remote(gb_send.at[s, p], gb_all.at[r, q], gb_ssem.at[s, p], gb_rsem.at[r, q], (rr, z * 2 + p)))
        else:
            for t in range(T):
                keep = jnp.where(q == 0, acc[t], acc[T + t])
                give = jnp.where(q == 0, acc[T + t], acc[t])
                gb_send[0, 0, t] = give.astype(BF16)
                gb_all[r, q, t] = keep.astype(BF16)
            push(remote(gb_send.at[0, 0], gb_all.at[r, q], gb_ssem.at[0, 0], gb_rsem.at[r, q], (r, other)))

    def total(buf, count):
        rows = []
        for t in range(T):
            for p in range(2):
                acc = buf[0, p, t].astype(F32)
                for n in range(1, count):
                    acc = acc + buf[n, p, t].astype(F32)
                rows.append(acc)
        return jnp.concatenate(rows, axis=0)

    def slot_wait(buf, sem, n, p):
        remote(buf.at[n, p], buf.at[n, p], dt_sem.at[0], sem.at[n, p], (r, other)).wait_recv()

    O = 2 * R
    chunk = 2 * H // O if fused else 0
    mid = Z // 2
    nearest = r * 2 + jnp.where(z >= mid, 1, 0)
    is_owner = (q == 1) & ((z == mid - 1) | (z == mid))

    def owner_device(o):
        return (o // 2, (mid - 1 + o % 2) * 2 + 1)

    def await_all(buf, count, ssem, rsem):
        part = buf.at[pl.ds(0, count)]
        return remote(part, part, ssem, rsem, (r, other))

    normt = normt_ref[...]

    def weight_part(m, g):
        part = jnp.dot(normt, g, preferred_element_type=F32)
        if fused:
            per = part.shape[0] // chunk
            at = (m % 2) * per
            wsend[m // 2, at : at + per] = part.astype(BF16).reshape(per, chunk, H)
        else:
            wgrad_ref[m] = part

    def spread(side):
        for s in range(1, O):
            o = lax.rem(nearest + s, O)
            remote(wsend.at[side, o], wrecv.at[side, me], ws_ssem.at[side], ws_rsem.at[side], owner_device(o)).start()

        @pl.when(is_owner)
        def _():
            wrecv[side, me] = wsend[side, nearest]

        @pl.when(jnp.logical_not(is_owner))
        def _():
            remote(wsend.at[side, nearest], wrecv.at[side, me], ws_ssem.at[side], ws_rsem.at[side], owner_device(nearest)).start()

    def collect(side):
        await_all(wrecv.at[side], N - 1, ws_ssem.at[side], ws_rsem.at[side]).wait_recv()
        acc = wrecv[side, 0].astype(F32)
        for n in range(1, N):
            acc = acc + wrecv[side, n].astype(F32)
        wback[side, nearest] = acc.astype(BF16)
        for s in range(1, N):
            d = lax.rem(me + s, N)
            remote(wback.at[side, nearest], wback.at[side, nearest], wb_ssem.at[side], wb_rsem.at[side], where(d)).start()

    def dn_part(m, g):
        return lax.dot_general(g, w_ref[m], (((1,), (1,)), ((), ())), preferred_element_type=F32)

    for s in list(range(1, Z)):
        zz = lax.rem(z + s, Z)
        for p in range(2):
            slot_wait(ga_all, ga_rsem, zz, p)
    slot_wait(ga_all, ga_rsem, z, 1 - q)
    left_grad = total(ga_all, Z)
    g = [(left_grad * coef[m]).astype(BF16) for m in range(2)]
    weight_part(0, g[0])
    weight_part(1, g[1])
    if fused:
        spread(0)
    dn = dn_part(0, g[0]) + dn_part(1, g[1])

    for s in list(range(1, R)):
        rr = lax.rem(r + s, R)
        for p in range(2):
            slot_wait(gb_all, gb_rsem, rr, p)
    slot_wait(gb_all, gb_rsem, r, 1 - q)
    right_grad = total(gb_all, R)
    g = [(right_grad * coef[m]).astype(BF16) for m in range(2, 4)]
    weight_part(2, g[0])
    weight_part(3, g[1])
    if fused:
        spread(1)
    dn = dn + dn_part(2, g[0]) + dn_part(3, g[1])

    xhat = xhat_ref[...]
    norm_part = jnp.concatenate(
        [jnp.sum(dn * xhat, axis=0, keepdims=True), jnp.sum(dn, axis=0, keepdims=True)], axis=0
    )
    if fused:
        nrecv[me] = norm_part
        for s in range(1, N):
            d = lax.rem(me + s, N)
            remote(nrecv.at[me], nrecv.at[me], n_ssem.at[0], n_rsem.at[0], where(d)).start()
    else:
        norm_ref[...] = norm_part
    dh = dn * gain_ref[...]
    grad = inv_ref[...] * (
        dh
        - jnp.mean(dh, axis=-1, keepdims=True)
        - xhat * jnp.mean(dh * xhat, axis=-1, keepdims=True)
    )
    pair_ref[...] = grad.astype(BF16).reshape(pair_ref.shape)

    if fused:

        @pl.when(is_owner)
        def _():
            collect(0)
            collect(1)

        await_all(nrecv, N - 1, n_ssem.at[0], n_rsem.at[0]).wait()
        acc = nrecv[0]
        for n in range(1, N):
            acc = acc + nrecv[n]
        norm_ref[...] = acc

        @pl.when(is_owner)
        def _():
            for side in range(2):
                await_all(wback.at[side], O - 1, ws_ssem.at[side], wb_rsem.at[side]).wait()
                await_all(wrecv.at[side], N - 1, wb_ssem.at[side], wb_rsem.at[side]).wait_send()

        @pl.when(jnp.logical_not(is_owner))
        def _():
            for side in range(2):
                await_all(wback.at[side], O, ws_ssem.at[side], wb_rsem.at[side]).wait()

        wgrad_ref[...] = wback[...].reshape(wgrad_ref.shape)
    for copy in sends:
        copy.wait_send()


def finish(pair_ref, wgrad_ref, norm_ref, pair_out, wgrad_out, norm_out, wide, sem):
    copies = [
        pltpu.make_async_copy(pair_ref, pair_out, sem.at[0]),
        pltpu.make_async_copy(norm_ref, norm_out, sem.at[1]),
    ]
    for copy in copies:
        copy.start()
    for m in range(wide.shape[0]):
        wide[m] = wgrad_ref[m].astype(F32)
        copies.append(pltpu.make_async_copy(wide.at[m], wgrad_out.at[m], sem.at[2 + m]))
        copies[-1].start()
    for copy in copies:
        copy.wait()


def on_device(R, C, z, dt, a, b, gain, bias, w):
    _, T, K, H = a.shape
    J = dt.shape[2]
    KH, Z, N = K // 2, C // 2, R * C
    fused = (4 * H) % (16 * N) == 0
    M, O = (N, 2 * R) if fused else (1, 1)
    chunk = 2 * H // O if fused else 8
    V = pltpu.VMEM
    D = pltpu.SemaphoreType.DMA
    anyspace = pl.BlockSpec(memory_space=pl.ANY)
    vspace = pl.BlockSpec(memory_space=pltpu.VMEM)
    pair, wgrad, norm = pl.pallas_call(
        functools.partial(kernel, R, C, fused),
        out_shape=(
            pltpu.VMEM(z.shape, BF16),
            pltpu.VMEM(w.shape, BF16 if fused else F32),
            pltpu.VMEM((2, z.shape[3]), F32),
        ),
        in_specs=[anyspace] * 7,
        out_specs=(vspace,) * 3,
        scratch_shapes=[
            V(z.shape, BF16),
            V(dt.shape, BF16),
            V(a.shape, BF16),
            V(b.shape, BF16),
            V((1, H), F32),
            V((1, H), F32),
            V(w.shape, BF16),
            V(dt.shape, BF16),
            V((2, C * T, J, H), F32),
            V((C * T, KH, H), BF16),
            V((2, J, KH, H), BF16),
            V((Z, 2, T, KH, H), BF16),
            V((R, 2, T, KH, H), BF16),
            V((Z, 2, T, KH, H), BF16),
            V((R, 2, T, KH, H), BF16),
            V((4, T * K, H), F32),
            V((T * K, H), F32),
            V((H, T * K), BF16),
            V((T * K, H), F32),
            V((2, O, chunk, H), BF16),
            V((2, M, chunk, H), BF16),
            V((2, O, chunk, H), BF16),
            V((M, 2, H), F32),
            D((7,)),
            D((2,)),
            D((C,)),
            D((C,)),
            D((R, 2)),
            D((R, 2)),
            D((Z, 2)),
            D((Z, 2)),
            D((R, 2)),
            D((R, 2)),
            D((2,)),
            D((2,)),
            D((2,)),
            D((2,)),
            D((1,)),
            D((1,)),
        ],
        compiler_params=pltpu.CompilerParams(
            collective_id=0, has_side_effects=True, vmem_limit_bytes=56 * 1024 * 1024
        ),
    )(z, dt, a, b, gain.reshape(1, -1), bias.reshape(1, -1), w)
    if not fused:
        wgrad, norm = lax.psum((wgrad, norm), ("row", "col"))
    return pl.pallas_call(
        finish,
        out_shape=(
            jax.ShapeDtypeStruct(z.shape, BF16),
            jax.ShapeDtypeStruct(w.shape, F32),
            jax.ShapeDtypeStruct(norm.shape, F32),
        ),
        in_specs=[vspace] * 3,
        out_specs=(anyspace,) * 3,
        scratch_shapes=[V(w.shape, F32), D((2 + w.shape[0],))],
        compiler_params=pltpu.CompilerParams(vmem_limit_bytes=4 * 1024 * 1024),
    )(pair, wgrad, norm)


def solution(mesh):
    R, C = mesh.shape["row"], mesh.shape["col"]
    return jax.shard_map(
        functools.partial(on_device, R, C),
        mesh=mesh,
        in_specs=(
            P("col", "row", None, None),
            P(None, "row", "col", None),
            P("col", "row", None, None),
            P("col", "row", None, None),
            P(),
            P(),
            P(),
        ),
        out_specs=(P("col", "row", None, None), P(), P()),
        check_vma=False,
    )
```
